32 devices in a mesh: aux: 4 (over y, x), pair: 8 (over z, core).
Axes of the slice: x: 2, y: 2, z: 4, core: 2. Of those that a mesh axis runs over, the one named last changes fastest.
Arguments:
- m_panels: bfloat16 [40000, 8192], P('aux', 'pair'), may hold values from -6 to 6
- lower_cols: bfloat16 [2, 512, 40000], P(None, 'pair', 'aux'), may hold values from -0.2 to 0.2, as said below
- diag_inverses: float32 [2, 512, 512], replicated, may hold values from -0.2 to 2, as said below
Outputs:
- remainder: bfloat16 [40000, 8192], P('aux', 'pair')
- solved: bfloat16 [2, 512, 8192], P(None, None, 'pair')
The draws below stay inside these ranges and needn't reach their ends.
Inputs may be any that keep to these rules, and one draw needn't show every extreme that they name: lower_cols[k] is zero in the pivot rows of panels 0 to k (the factor is lower triangular and its diagonal blocks are given by their inverses). Each diag_inverses[k] is lower triangular.
All inputs are finite; a program needn't handle non-finite values.
Results may differ from the reference program's by a relative error of at most 0.0047.
Values may be sent and summed in bfloat16 or wider, within the bound.
A program may use at most 192 MiB of HBM per device.

```python
import jax
import jax.numpy as jnp
from jax import lax

NAUX = 40000
NB = 512
PANELS = 2
PAIR_DEV = 1024
AUX_ROWS = 10000
NPAIR = 8192
N_PAIR = 8


def draw_lower_cols(key, part):
    scale = 1.0 / (PANELS * NB) ** 0.5
    values = jnp.clip(jax.random.normal(key, (PANELS, NB, NAUX), jnp.float32), -6.0, 6.0)
    rows = jnp.arange(NAUX, dtype=jnp.int32)
    block = rows // AUX_ROWS
    within = rows % AUX_ROWS
    panel = jnp.arange(PANELS, dtype=jnp.int32)[:, None]
    keep = jnp.logical_not(jnp.logical_and(within[None, :] < NB, block[None, :] <= panel))
    values = jnp.clip(values * scale, -0.199, 0.199) * keep.astype(jnp.float32)[:, None, :]
    return values.astype(jnp.bfloat16)


def draw_diag_inverses(key, part):
    first = jax.random.fold_in(key, 11)
    second = jax.random.fold_in(key, 12)
    lower = jnp.clip(jax.random.normal(first, (PANELS, NB, NB), jnp.float32), -6.0, 6.0)
    lower = jnp.clip(lower * (0.7 / NB ** 0.5), -0.199, 0.199) * jnp.tril(jnp.ones((NB, NB), jnp.float32), -1)[None]
    diagonal = jnp.exp(jax.random.uniform(second, (PANELS, NB), jnp.float32, -0.69, 0.69))
    return lower + diagonal[:, :, None] * jnp.eye(NB, dtype=jnp.float32)[None]


def levels(own_key, extent, split, smallest, high):
    factor_of, own = 1.0, jax.random.fold_in(own_key, 6)
    for dim, parts in split:
        heights = jnp.exp(jax.random.uniform(jax.random.fold_in(own, dim), (parts,), jnp.float32, smallest / len(split), high / len(split)))
        factor_of = factor_of * jnp.repeat(heights, extent[dim] // parts).reshape([-1 if axis == dim else 1 for axis in range(len(extent))])
    return factor_of


def scatter_about(rng, extent, spread, most, split=(), held_as=jnp.bfloat16):
    drawn = spread * jax.random.normal(rng, extent, jnp.float32)
    if split:
        drawn = drawn * levels(rng, extent, split, -0.22, 0.18)
    return jnp.clip(drawn, -most, most).astype(held_as)


def setup_inputs(seed: int = 0) -> dict:
    key_list = jax.random.split(jax.random.key(seed), 4)
    m_panels = scatter_about(key_list[0], (NAUX, NPAIR), 1.0, 6.0, ((0, 4), (1, 8)))
    lower_cols = draw_lower_cols(jax.random.fold_in(key_list[3], 71), 0)
    diag_inverses = draw_diag_inverses(jax.random.fold_in(key_list[3], 71), 0)
    return dict(m_panels=m_panels, lower_cols=lower_cols, diag_inverses=diag_inverses)


def one_group(block_cols, lower_cols, diag_inverses):
    work = block_cols.astype(jnp.float32)
    results = []
    for panel in range(PANELS):
        first = panel * AUX_ROWS
        pivot = work[first:first + NB]
        solved_rows = jnp.dot(diag_inverses[panel], pivot, precision=lax.Precision.HIGHEST, preferred_element_type=jnp.float32).astype(jnp.bfloat16)
        work = work - jnp.dot(lower_cols[panel].T, solved_rows, preferred_element_type=jnp.float32)
        results.append(solved_rows)
    return work.astype(jnp.bfloat16), jnp.stack(results)


def reference(m_panels, lower_cols, diag_inverses):
    groups = m_panels.reshape(NAUX, N_PAIR, PAIR_DEV).transpose(1, 0, 2)
    remains, solves = lax.map(lambda cols: one_group(cols, lower_cols, diag_inverses), groups)
    remainder = remains.transpose(1, 0, 2).reshape(NAUX, N_PAIR * PAIR_DEV)
    solved = solves.transpose(1, 2, 0, 3).reshape(PANELS, NB, N_PAIR * PAIR_DEV)
    return remainder, solved
```

```python
import functools

import jax
import jax.numpy as jnp
from jax import lax
from jax.experimental import pallas as pl
from jax.experimental.pallas import tpu as pltpu
from jax.sharding import PartitionSpec as P

CHUNKS = 10
TILE = 256
CORES = 2
CONTRACT = (((0,), (0,)), ((), ()))
MESH = pl.DeviceIdType.MESH


def kernel(aux, chips, chunks, chunk, m_hbm, l_hbm, l_tail, dinv_ref, mbuf, solved_ref,
           lbuf, sbuf, load_sem, ring_sem, swap_sem, left_sem, right_sem, part_sem,
           srecv_sem, ssend_sem):
    rows, columns = m_hbm.shape
    panels, width = dinv_ref.shape[:2]
    even = rows - rows % TILE
    padded = lbuf.shape[-1]
    a = lax.axis_index("aux")
    me = lax.axis_index("pair")
    z, c = me // CORES, lax.rem(me, CORES)
    to_left = {"pair": lax.rem(z + chips - 1, chips) * CORES + c}
    to_right = {"pair": lax.rem(z + 1, chips) * CORES + c}
    partner = {"pair": z * CORES + 1 - c}

    own_load = pltpu.make_async_copy(
        l_hbm.at[:, :, pl.ds(0, even)], lbuf.at[me, :, :, pl.ds(0, even)], load_sem.at[0])
    own_tail = pltpu.make_async_copy(
        l_tail, lbuf.at[me, :, :, pl.ds(even, padded - even)], load_sem.at[3])
    pivot_load = pltpu.make_async_copy(
        m_hbm.at[pl.ds(0, width)], mbuf.at[pl.ds(0, width)], load_sem.at[1])
    rest_load = pltpu.make_async_copy(
        m_hbm.at[pl.ds(width, rows - width)], mbuf.at[pl.ds(width, rows - width)], load_sem.at[2])
    own_load.start()
    own_tail.start()
    pivot_load.start()

    barrier = pltpu.get_barrier_semaphore()
    for peer in (to_left, to_right, partner):
        pl.semaphore_signal(barrier, inc=1, device_id=peer, device_id_type=MESH)
    for step in range(1, aux):
        peer = {"aux": lax.rem(a + step, aux)}
        pl.semaphore_signal(barrier, inc=1, device_id=peer, device_id_type=MESH)
    pl.semaphore_wait(barrier, 2 + aux)
    own_load.wait()
    own_tail.wait()
    rest_load.start()

    def piece(block, j):
        return lbuf.at[block, :, :, pl.ds(pl.multiple_of(j * chunk, 128), chunk)]

    def ring(zb, j, send, peer):
        ref = piece(zb * CORES + c, j)
        return pltpu.make_async_remote_copy(
            src_ref=ref, dst_ref=ref, send_sem=send.at[zb, j], recv_sem=ring_sem.at[zb, j],
            device_id=peer, device_id_type=MESH)

    def swap(zb, j, core):
        ref = piece(zb * CORES + core, j)
        return pltpu.make_async_remote_copy(
            src_ref=ref, dst_ref=ref, send_sem=part_sem.at[zb, j], recv_sem=swap_sem.at[zb, j],
            device_id=partner, device_id_type=MESH)

    def solve(panel):
        def columns_of(i, _):
            cols = pl.ds(pl.multiple_of(i * TILE, TILE), TILE)
            pivot = mbuf[pl.ds(0, width), cols].astype(jnp.float32)
            for before in range(panel):
                factor = lbuf[:, before, :, pl.ds(0, width)].reshape(-1, width)
                pivot = pivot - lax.dot_general(
                    factor, sbuf[before, :, cols], CONTRACT, preferred_element_type=jnp.float32)
            sbuf[panel, :, cols] = jnp.dot(
                dinv_ref[panel], pivot, precision=lax.Precision.HIGHEST,
                preferred_element_type=jnp.float32).astype(jnp.bfloat16)
            return 0

        lax.fori_loop(0, columns // TILE, columns_of, 0)

    def spread(panel, step):
        return pltpu.make_async_remote_copy(
            src_ref=sbuf.at[panel], dst_ref=sbuf.at[panel],
            send_sem=ssend_sem.at[panel, step], recv_sem=srecv_sem.at[panel],
            device_id={"aux": lax.rem(a + step, aux)}, device_id_type=MESH)

    def settle(panel):
        solve(panel)
        for step in range(1, aux):
            spread(panel, step).start()

    def product(here):
        return sum(
            lax.dot_general(
                lbuf[:, panel, :, here].reshape(-1, TILE), sbuf[panel], CONTRACT,
                preferred_element_type=jnp.float32)
            for panel in range(panels))

    def update(j):
        def tile(i, _):
            here = pl.ds(pl.multiple_of(i * TILE, TILE), TILE)
            mbuf[here] = (mbuf[here].astype(jnp.float32) - product(here)).astype(jnp.bfloat16)
            return 0

        tiles = chunk // TILE
        lax.fori_loop(j * tiles, jnp.minimum((j + 1) * tiles, even // TILE), tile, 0)

    def complete(j):
        for zb in range(chips):
            swap(zb, j, 1 - c).wait_recv()

    def tick(t):
        @pl.when(t < chunks)
        def _():
            @pl.when(z > 0)
            def _():
                ring(z, t, left_sem, to_left).start()

            @pl.when(z < chips - 1)
            def _():
                ring(z, t, right_sem, to_right).start()

            swap(z, t, c).start()

        for step in range(1, chips):
            j = t - step
            live = jnp.logical_and(j >= 0, j < chunks)

            @pl.when(jnp.logical_and(live, z + step < chips))
            def _():
                ring(z + step, j, left_sem, to_left).wait_recv()

                @pl.when(z > 0)
                def _():
                    ring(z + step, j, left_sem, to_left).start()

                swap(z + step, j, c).start()

            @pl.when(jnp.logical_and(live, z >= step))
            def _():
                ring(z - step, j, right_sem, to_right).wait_recv()

                @pl.when(z < chips - 1)
                def _():
                    ring(z - step, j, right_sem, to_right).start()

                swap(z - step, j, c).start()

        j = t - (chips - 1)

        @pl.when(jnp.logical_and(j >= 0, j < chunks))
        def _():
            complete(j)

    first = max(chips + panels, chunks // 2 + chips)
    last = chunks + chips - 1

    def ticks(t, _):
        tick(t)
        return 0

    tick(jnp.int32(0))
    pivot_load.wait()

    @pl.when(a == 0)
    def _():
        settle(0)

    lax.fori_loop(1, chips, ticks, 0)
    for panel in range(1, panels):
        @pl.when(a == panel)
        def _(panel=panel):
            for before in range(panel):
                spread(before, 1).wait_recv()
            settle(panel)

        lax.fori_loop(chips - 1 + panel, chips + panel, ticks, 0)
    lax.fori_loop(chips - 1 + panels, first, ticks, 0)

    for panel in range(panels):
        @pl.when(jnp.logical_and(a != panel, jnp.logical_or(a < panel, a >= panels)))
        def _(panel=panel):
            spread(panel, 1).wait_recv()
    rest_load.wait()
    solved_ref[...] = sbuf[...]

    def updates(j, _):
        update(j)
        return 0

    lax.fori_loop(0, first - chips + 1, updates, 0)

    def both(t, _):
        tick(t)
        update(t - (chips - 1))
        return 0

    lax.fori_loop(first, last, both, 0)

    if even < rows:
        left = rows - even
        here = pl.ds(even, left)
        total = mbuf[here].astype(jnp.float32) - product(pl.ds(even, TILE))[:left]
        mbuf[here] = total.astype(jnp.bfloat16)

    def drain(j, _):
        for zb in range(chips):
            @pl.when(jnp.logical_and(z > 0, z <= zb))
            def _():
                ring(jnp.int32(zb), j, left_sem, to_left).wait_send()

            @pl.when(jnp.logical_and(z < chips - 1, z >= zb))
            def _():
                ring(jnp.int32(zb), j, right_sem, to_right).wait_send()

            swap(jnp.int32(zb), j, c).wait_send()
        return 0

    lax.fori_loop(0, chunks, drain, 0)
    for panel in range(panels):
        @pl.when(a == panel)
        def _(panel=panel):
            for step in range(1, aux):
                spread(panel, step).wait_send()


def shards(aux, pair, m_panels, lower_cols, diag_inverses):
    panels, width = diag_inverses.shape[:2]
    rows, columns = m_panels.shape
    part = lower_cols.shape[1]
    chips = pair // CORES
    chunk = max(-(-rows // (CHUNKS * TILE)), -(-width // TILE)) * TILE
    chunks = -(-rows // chunk)
    padded = chunks * chunk
    even = rows - rows % TILE
    tail = jnp.pad(lower_cols[:, :, even:], ((0, 0), (0, 0), (0, padded - rows)))
    anywhere = pl.BlockSpec(memory_space=pl.ANY)
    vmem = pl.BlockSpec(memory_space=pltpu.VMEM)
    dma = pltpu.SemaphoreType.DMA
    return pl.pallas_call(
        functools.partial(kernel, aux, chips, chunks, chunk),
        in_specs=[anywhere, anywhere, anywhere, vmem],
        out_specs=[vmem, vmem],
        out_shape=[
            pltpu.VMEM((rows, columns), jnp.bfloat16),
            jax.ShapeDtypeStruct((panels, width, columns), jnp.bfloat16),
        ],
        scratch_shapes=[
            pltpu.VMEM((pair, panels, part, padded), jnp.bfloat16),
            pltpu.VMEM((panels, width, columns), jnp.bfloat16),
            dma((4,)),
            dma((chips, chunks)),
            dma((chips, chunks)),
            dma((chips, chunks)),
            dma((chips, chunks)),
            dma((chips, chunks)),
            dma((panels,)),
            dma((panels, aux)),
        ],
        compiler_params=pltpu.CompilerParams(
            collective_id=0, has_side_effects=True, vmem_limit_bytes=40 * 1024 * 1024),
    )(m_panels, lower_cols, tail, diag_inverses)


def solution(mesh):
    placed = (P("aux", "pair"), P(None, "pair", "aux"), P())
    return jax.shard_map(
        functools.partial(shards, mesh.shape["aux"], mesh.shape["pair"]),
        mesh=mesh,
        in_specs=placed,
        out_specs=(P("aux", "pair"), P(None, None, "pair")),
        check_vma=False,
    )
```
